32 devices in a mesh: section: 8 (over z, x), fsdp: 4 (over y, core).
Axes of the slice: x: 2, y: 2, z: 4, core: 2. Of those that a mesh axis runs over, the one named last changes fastest.
Arguments:
- layer_inputs: bfloat16 [8, 2, 1536, 2048], P('section', None, 'fsdp'), may hold values from -6 to 6
- out_grads: bfloat16 [8, 2, 1536, 2048], P('section', None, 'fsdp'), may hold values from -6 to 6
- attn_stash: bfloat16 [8, 2, 1536, 1024], P('section', None, 'fsdp'), may hold values from -6 to 6
- proj_grads: bfloat16 [8, 2, 1536, 1536], P('section', None, 'fsdp'), may hold values from -6 to 6
- w_qkv: bfloat16 [8, 2048, 1536], P('section', 'fsdp'), may hold values from -0.125 to 0.125
- w_out: bfloat16 [8, 1024, 2048], P('section', 'fsdp'), may hold values from -0.1875 to 0.1875
- norm_gain: float32 [8, 2048], P('section'), may hold values from 0.25 to 1.75
- b_sched: int32 [8], P('section'), may hold values from 0 to 1
- w_sched: int32 [8], P('section'), may hold values from 0 to 1
Outputs:
- prev_grads: bfloat16 [8, 1536, 2048], P('section', 'fsdp')
- grad_qkv: float32 [8, 2048, 1536], P('section', 'fsdp')
- grad_out: float32 [8, 1024, 2048], P('section', 'fsdp')
The draws below stay inside these ranges and needn't reach their ends.
All inputs are finite; a program needn't handle non-finite values.
Results may differ from the reference program's by a relative error of at most 0.012.
Values may be sent and summed in bfloat16 or wider, within the bound.
A program may use at most 128 MiB of HBM per device.

```python
import jax
import jax.numpy as jnp
from jax import lax

D = 2048
HEAD_DIM = 64
HEADS = 16
KV_HEADS = 4
SEQ = 384
MICRO = 2
SECTIONS = 8
Q_WIDTH = 1024
QKV_WIDTH = 1536
TOKENS = 1536
N_FSDP = 4


def set_ends(values, own_key, smallest, top_value):
    longest = values.shape.index(max(values.shape))
    spots = []
    for shift in (0, 1):
        where = [jax.random.randint(jax.random.fold_in(own_key, axis), (), 0, length) for axis, length in enumerate(values.shape)]
        where[longest] = (where[longest] + shift) % values.shape[longest]
        spots.append(tuple(where))
    return values.at[spots[0]].set(smallest).at[spots[1]].set(top_value)


def raised(values, stream_key, source, target, parts, factor):
    owner, partner = [(jnp.arange(values.shape[position]) // (values.shape[position] // parts)).reshape([-1 if axis == position else 1 for axis in range(values.ndim)]) for position in (source, target)]
    chosen = jax.random.permutation(stream_key, parts)[partner]
    strong = (owner == chosen) | (owner == (partner + parts // 2) % parts)
    return jnp.where(strong, factor * values, values)


def level_of(own_key, shape, cuts, smallest, high):
    def one(axis_at, blocks):
        steps = jax.random.uniform(jax.random.fold_in(jax.random.fold_in(own_key, 6), axis_at), (blocks,), jnp.float32, smallest / len(cuts), high / len(cuts))
        return jnp.repeat(jnp.exp(steps), shape[axis_at] // blocks).reshape((-1,) + (1,) * (len(shape) - axis_at - 1))

    loudness = one(*cuts[0])
    for cut in cuts[1:]:
        loudness = loudness * one(*cut)
    return loudness


def scatter_about(stream_key, dims, scale, bound, pieces=(), kind=jnp.bfloat16):
    loudness = level_of(stream_key, dims, pieces, -0.22, 0.18) if pieces else 1.0
    entries = jax.random.normal(stream_key, dims, jnp.float32) * scale * loudness
    return jnp.minimum(jnp.maximum(entries, -bound), bound).astype(kind)


def heavy_noise(key, dims, spread, most, pieces, heavy, kind=jnp.bfloat16):
    entries = spread * jax.random.normal(key, dims, jnp.float32)
    if pieces:
        entries = entries * level_of(key, dims, pieces, -0.22, 0.18)
    return jnp.clip(raised(entries, jax.random.fold_in(key, 3), *heavy), -most, most).astype(kind)


def setup_inputs(seed: int = 0) -> dict:
    streams_of = jax.random.split(jax.random.key(seed), 10)
    layer_inputs = scatter_about(streams_of[0], (SECTIONS, MICRO, TOKENS, D), 1.0, 6.0, ((0, 8), (2, 4)))
    out_grads = scatter_about(streams_of[1], (SECTIONS, MICRO, TOKENS, D), 1.0, 6.0, ((0, 8), (2, 4)))
    attn_stash = heavy_noise(streams_of[2], (SECTIONS, MICRO, TOKENS, Q_WIDTH), 1.0, 6.0, ((0, 8), (2, 4)), (2, 3, 4, 2.0))
    proj_grads = scatter_about(streams_of[3], (SECTIONS, MICRO, TOKENS, QKV_WIDTH), 1.0, 6.0, ((0, 8), (2, 4)))
    w_qkv = scatter_about(streams_of[4], (SECTIONS, D, QKV_WIDTH), D ** -0.5, 0.125, ((0, 8), (1, 4)))
    w_out = scatter_about(streams_of[5], (SECTIONS, Q_WIDTH, D), Q_WIDTH ** -0.5, 0.1875, ((0, 8), (1, 4)))
    norm_gain = jnp.clip(1.0 + 0.15 * jax.random.normal(streams_of[6], (SECTIONS, D), jnp.float32), 0.25, 1.75)
    b_sched = set_ends(jax.random.randint(streams_of[7], (SECTIONS,), 0, MICRO), jax.random.fold_in(streams_of[7], 1), 0, MICRO - 1).astype(jnp.int32)
    w_sched = set_ends(jax.random.randint(streams_of[8], (SECTIONS,), 0, MICRO), jax.random.fold_in(streams_of[8], 1), 0, MICRO - 1).astype(jnp.int32)
    return dict(layer_inputs=layer_inputs, out_grads=out_grads, attn_stash=attn_stash, proj_grads=proj_grads, w_qkv=w_qkv, w_out=w_out, norm_gain=norm_gain, b_sched=b_sched, w_sched=w_sched)


rms_eps = 1e-05
rope_base = 500000.0

def rope_tables(length, head_size):
    halfway = head_size // 2
    indices = jnp.arange(halfway, dtype=jnp.float32)
    frequency = rope_base ** (-2.0 * indices / head_size)
    angles = jnp.arange(length, dtype=jnp.float32)[:, None] * frequency[None, :]
    angles = jnp.concatenate([angles, angles], axis=1)
    return (jnp.cos(angles), jnp.sin(angles))

def rotate_half(values):
    halfway = values.shape[-1] // 2
    return jnp.concatenate([-values[..., halfway:], values[..., :halfway]], axis=-1)

def apply_rope(values, cosine_table, sine_table):
    return values * cosine_table[:, None, :] + rotate_half(values) * sine_table[:, None, :]

def unapply_rope(values, cosine_table, sine_table):
    return values * cosine_table[:, None, :] - rotate_half(values * sine_table[:, None, :])

def contract(pattern, first_operand, second_operand):
    return jnp.einsum(pattern, first_operand.astype(jnp.float32), second_operand.astype(jnp.float32))

def normalize(inputs, gain_values):
    widened = inputs.astype(jnp.float32)
    inv_rms = lax.rsqrt(lax.optimization_barrier(jnp.mean(widened * widened, axis=-1, keepdims=True)) + rms_eps)
    normed = (widened * inv_rms * gain_values).astype(jnp.bfloat16)
    return (widened, inv_rms, normed)

def attention_back(qkv_rows, attn_grad, cosine_table, sine_table):
    tokens_here = qkv_rows.shape[0]
    q_width = HEADS * HEAD_DIM
    kv_width = KV_HEADS * HEAD_DIM
    group_size = HEADS // KV_HEADS
    score_scale = HEAD_DIM ** (-0.5)
    queries = apply_rope(qkv_rows[:, :q_width].reshape(tokens_here, HEADS, HEAD_DIM), cosine_table, sine_table).astype(jnp.bfloat16)
    key_heads = apply_rope(qkv_rows[:, q_width:q_width + kv_width].reshape(tokens_here, KV_HEADS, HEAD_DIM), cosine_table, sine_table).astype(jnp.bfloat16)
    values = qkv_rows[:, q_width + kv_width:].reshape(tokens_here, KV_HEADS, HEAD_DIM).astype(jnp.bfloat16)
    queries = queries.reshape(tokens_here, KV_HEADS, group_size, HEAD_DIM)
    grad_heads = attn_grad.reshape(tokens_here, KV_HEADS, group_size, HEAD_DIM)
    scores = contract('tkgd,ukd->kgtu', queries, key_heads) * score_scale
    row_ids = lax.broadcasted_iota(jnp.int32, (tokens_here, tokens_here), 0)
    col_ids = lax.broadcasted_iota(jnp.int32, (tokens_here, tokens_here), 1)
    causal = col_ids <= row_ids
    exp_scores = jnp.where(causal, jnp.exp(scores), 0.0)
    attention = exp_scores / lax.optimization_barrier(jnp.sum(exp_scores, axis=-1, keepdims=True))
    attention_low = attention.astype(jnp.bfloat16)
    grad_values = contract('kgtu,tkgd->ukd', attention_low, grad_heads)
    grad_attention = contract('tkgd,ukd->kgtu', grad_heads, values)
    row_delta = lax.optimization_barrier(jnp.sum(attention * grad_attention, axis=-1, keepdims=True))
    grad_scores = (attention * (grad_attention - row_delta) * score_scale).astype(jnp.bfloat16)
    grad_queries = contract('kgtu,ukd->tkgd', grad_scores, key_heads)
    grad_keys = contract('kgtu,tkgd->ukd', grad_scores, queries)
    grad_queries = unapply_rope(grad_queries.reshape(tokens_here, HEADS, HEAD_DIM), cosine_table, sine_table)
    grad_keys = unapply_rope(grad_keys, cosine_table, sine_table)
    joined = jnp.concatenate([grad_queries.reshape(tokens_here, q_width), grad_keys.reshape(tokens_here, kv_width), grad_values.reshape(tokens_here, kv_width)], axis=1)
    return joined.astype(jnp.bfloat16)

def finish_grad(widened, inv_rms, gain_values, upstream, grad_normed):
    scaled = grad_normed * gain_values
    inner_mean = lax.optimization_barrier(jnp.mean(scaled * widened, axis=-1, keepdims=True))
    result = upstream.astype(jnp.float32) + inv_rms * scaled - widened * inv_rms ** 3 * inner_mean
    return result.astype(jnp.bfloat16)

def reference(layer_inputs, out_grads, attn_stash, proj_grads, w_qkv, w_out, norm_gain, b_sched, w_sched):
    cosine_table, sine_table = rope_tables(SEQ, HEAD_DIM)
    contract_rows = (((0,), (0,)), ((), ()))
    contract_cols = (((1,), (1,)), ((), ()))

    def one_section(operands):
        inputs, upstream, attended, projected, weight_qkv, weight_out, gain_values, b_slot, w_slot = operands
        inputs_b = lax.dynamic_index_in_dim(inputs, b_slot, 0, keepdims=False).reshape(N_FSDP, SEQ, D)
        upstream_b = lax.dynamic_index_in_dim(upstream, b_slot, 0, keepdims=False).reshape(N_FSDP, SEQ, D)

        def one_sequence(seq_pair):
            seq_inputs, seq_upstream = seq_pair
            widened, inv_rms, normed = normalize(seq_inputs, gain_values)
            qkv_rows = jnp.dot(normed, weight_qkv, preferred_element_type=jnp.float32)
            attn_grad = lax.dot_general(seq_upstream, weight_out, contract_cols, preferred_element_type=jnp.float32).astype(jnp.bfloat16)
            grad_proj = attention_back(qkv_rows, attn_grad, cosine_table, sine_table)
            grad_normed = lax.dot_general(grad_proj, weight_qkv, contract_cols, preferred_element_type=jnp.float32)
            return finish_grad(widened, inv_rms, gain_values, seq_upstream, grad_normed)
        sent_grads = lax.map(one_sequence, (inputs_b, upstream_b)).reshape(TOKENS, D)
        inputs_w = lax.dynamic_index_in_dim(inputs, w_slot, 0, keepdims=False).reshape(N_FSDP, SEQ, D)
        upstream_w = lax.dynamic_index_in_dim(upstream, w_slot, 0, keepdims=False).reshape(N_FSDP, SEQ, D)
        attended_w = lax.dynamic_index_in_dim(attended, w_slot, 0, keepdims=False).reshape(N_FSDP, SEQ, Q_WIDTH)
        projected_w = lax.dynamic_index_in_dim(projected, w_slot, 0, keepdims=False).reshape(N_FSDP, SEQ, QKV_WIDTH)

        def add_member(totals, member):
            m_inputs, m_upstream, m_attended, m_projected = member
            unused_wide, unused_inv, normed = normalize(m_inputs, gain_values)
            part_qkv = lax.dot_general(normed, m_projected, contract_rows, preferred_element_type=jnp.float32)
            part_out = lax.dot_general(m_attended, m_upstream, contract_rows, preferred_element_type=jnp.float32)
            part_qkv = lax.optimization_barrier(part_qkv.astype(jnp.bfloat16)).astype(jnp.float32)
            part_out = lax.optimization_barrier(part_out.astype(jnp.bfloat16)).astype(jnp.float32)
            return ((totals[0] + part_qkv, totals[1] + part_out), None)
        zero_totals = (jnp.zeros((D, QKV_WIDTH), jnp.float32), jnp.zeros((Q_WIDTH, D), jnp.float32))
        grad_pair, unused_out = lax.scan(add_member, zero_totals, (inputs_w, upstream_w, attended_w, projected_w))
        return (sent_grads, grad_pair[0], grad_pair[1])
    sent_all, grad_qkv, grad_out = lax.map(one_section, (layer_inputs, out_grads, attn_stash, proj_grads, w_qkv, w_out, norm_gain, b_sched, w_sched))
    return (jnp.roll(sent_all, -1, axis=0), grad_qkv, grad_out)
```

```python
import jax
import jax.numpy as jnp
from jax import lax
from jax.experimental import pallas as pl
from jax.experimental.pallas import tpu as pltpu
from jax.sharding import PartitionSpec as P

HEAD_DIM = 64
HEADS = 16
KV_HEADS = 4


rms_eps = 1e-05
rope_base = 500000.0


def passed_along(array, axis, by):
    size = lax.axis_size(axis)
    return lax.ppermute(array, axis, [(i, (i + by) % size) for i in range(size)])


def rope_tables(length, head_size):
    halfway = head_size // 2
    indices = jnp.arange(halfway, dtype=jnp.float32)
    frequency = rope_base ** (-2.0 * indices / head_size)
    angles = jnp.arange(length, dtype=jnp.float32)[:, None] * frequency[None, :]
    angles = jnp.concatenate([angles, angles], axis=1)
    return (jnp.cos(angles), jnp.sin(angles))


def pair_tables(length):
    cosine_table, sine_table = rope_tables(length, HEAD_DIM)
    low_half = jnp.arange(HEAD_DIM)[None, :] < HEAD_DIM // 2
    signed = jnp.where(low_half, -sine_table, sine_table)
    return (jnp.tile(cosine_table, (1, 2)), jnp.tile(signed, (1, 2)))


def attention_kernel(q_ref, k_ref, v_ref, g_ref, cos_ref, sin_ref, o_ref, gk_ref, gv_ref):
    step = pl.program_id(0)
    length = q_ref.shape[0]
    pair = 2 * HEAD_DIM
    half = HEAD_DIM // 2
    q_width = HEADS * HEAD_DIM
    kv_width = KV_HEADS * HEAD_DIM
    group = HEADS // KV_HEADS
    score_scale = HEAD_DIM ** (-0.5)
    lane = lax.broadcasted_iota(jnp.int32, (length, pair), 1)
    low = lane % HEAD_DIM < half
    left = lane < HEAD_DIM
    edges = (0, 128, length) if length > 128 else (0, length)

    def swapped(u):
        return jnp.where(low, pltpu.roll(u, pair - half, 1), pltpu.roll(u, half, 1))

    def rope(u):
        return u * cos_ref[...] + swapped(u) * sin_ref[...]

    def unrope(u):
        return u * cos_ref[...] - swapped(u) * sin_ref[...]

    def rows(a, b):
        return lax.dot_general(a, b, (((1,), (1,)), ((), ())), preferred_element_type=jnp.float32)

    def dot(a, b):
        return jnp.dot(a, b, preferred_element_type=jnp.float32)

    def both_sides(u, which):
        mine = jnp.where(left if which == 0 else ~left, u, 0.0)
        other = pltpu.roll(mine, HEAD_DIM, 1)
        return (mine, other) if which == 0 else (other, mine)

    keys = rope(k_ref[...])
    values = v_ref[...]
    summed = []
    for which in range(2):
        key_sides = both_sides(keys, which)
        key_low = [u.astype(jnp.bfloat16) for u in key_sides]
        key_turned = [u.T.astype(jnp.bfloat16) for u in key_sides]
        value_low = [u.astype(jnp.bfloat16) for u in both_sides(values, which)]
        gk_ref[...] = jnp.zeros_like(gk_ref)
        gv_ref[...] = jnp.zeros_like(gv_ref)
        for number in range(group // 2):
            at = (which * (group // 2) + number) * pair
            query = (rope(q_ref[:, at : at + pair]) * score_scale).astype(jnp.bfloat16)
            grads = g_ref[:, at : at + pair]
            turned = []
            for start, stop in zip(edges[:-1], edges[1:]):
                query_part = query[start:stop]
                grads_part = grads[start:stop]
                seen = lax.broadcasted_iota(
                    jnp.int32, (stop, stop - start), 0
                ) <= start + lax.broadcasted_iota(jnp.int32, (stop, stop - start), 1)
                total = 0.0
                for side in range(2):
                    raised = jnp.where(
                        seen, jnp.exp(rows(key_low[side][:stop], query_part)), 0.0
                    )
                    probs = raised * (1.0 / jnp.sum(raised, axis=0, keepdims=True))
                    grad_probs = rows(value_low[side][:stop], grads_part)
                    weighted = probs * grad_probs
                    delta = jnp.sum(weighted, axis=0, keepdims=True)
                    grad_scores = (weighted - probs * delta).astype(jnp.bfloat16)
                    gv_ref[side, :stop] += dot(probs.astype(jnp.bfloat16), grads_part)
                    gk_ref[side, :stop] += dot(grad_scores, query_part)
                    total = total + dot(key_turned[side][:, :stop], grad_scores)
                turned.append(total)
            grad_query = jnp.concatenate(turned, axis=1).T * score_scale
            where = pl.multiple_of(step * (group * pair) + at, pair)
            o_ref[:, pl.ds(where, pair)] = unrope(grad_query).astype(o_ref.dtype)
        for_keys = jnp.where(left, gk_ref[0], gk_ref[1])
        for_values = jnp.where(left, gv_ref[0], gv_ref[1])
        summed.append(
            (
                for_keys + pltpu.roll(for_keys, HEAD_DIM, 1),
                for_values + pltpu.roll(for_values, HEAD_DIM, 1),
            )
        )
    grad_keys = unrope(jnp.where(left, summed[0][0], summed[1][0]))
    grad_values = jnp.where(left, summed[0][1], summed[1][1])
    where = pl.multiple_of(q_width + step * pair, pair)
    o_ref[:, pl.ds(where, pair)] = grad_keys.astype(o_ref.dtype)
    where = pl.multiple_of(q_width + kv_width + step * pair, pair)
    o_ref[:, pl.ds(where, pair)] = grad_values.astype(o_ref.dtype)


def attention_back(qkv_rows, attn_grad, cosine_table, sine_table):
    length, width = qkv_rows.shape
    pair = 2 * HEAD_DIM
    q_block = HEADS // KV_HEADS * pair
    k_at = HEADS * HEAD_DIM // pair
    v_at = k_at + KV_HEADS * HEAD_DIM // pair
    table = pl.BlockSpec((length, pair), lambda p: (0, 0))
    return pl.pallas_call(
        attention_kernel,
        grid=(KV_HEADS // 2,),
        out_shape=jax.ShapeDtypeStruct((length, width), jnp.bfloat16),
        in_specs=[
            pl.BlockSpec((length, q_block), lambda p: (0, p)),
            pl.BlockSpec((length, pair), lambda p: (0, k_at + p)),
            pl.BlockSpec((length, pair), lambda p: (0, v_at + p)),
            pl.BlockSpec((length, q_block), lambda p: (0, p)),
            table,
            table,
        ],
        out_specs=pl.BlockSpec((length, width), lambda p: (0, 0)),
        scratch_shapes=[
            pltpu.VMEM((2, length, pair), jnp.float32),
            pltpu.VMEM((2, length, pair), jnp.float32),
        ],
        compiler_params=pltpu.CompilerParams(
            dimension_semantics=("arbitrary",), vmem_limit_bytes=32 * 1024 * 1024
        ),
        cost_estimate=pl.CostEstimate(
            flops=40 * length * length * HEADS * HEAD_DIM,
            bytes_accessed=12 * length * width,
            transcendentals=length * length * HEADS,
        ),
        name="attention_back",
    )(qkv_rows, qkv_rows, qkv_rows, attn_grad, cosine_table, sine_table)


def across_cores(array):
    size = lax.axis_size("fsdp")
    return lax.ppermute(array, "fsdp", [(i, i ^ 1) for i in range(size)])


def across_chips(array, by):
    size = lax.axis_size("fsdp")
    return lax.ppermute(array, "fsdp", [(i, (i + 2 * by) % size) for i in range(size)])


def gathered(shard, pieces):
    size = lax.axis_size("fsdp")
    me = lax.axis_index("fsdp")
    rows = shard.shape[0]
    cut = rows // pieces
    arrived = [
        ((me + size - 2 * by) % size, i, across_chips(shard[i * cut : (i + 1) * cut], by))
        for i in range(pieces)
        for by in range(1, size // 2)
    ]
    found = [(me * rows, shard), ((me ^ 1) * rows, across_cores(shard))]
    for owner, i, part in arrived:
        found.append((owner * rows + i * cut, part))
        found.append(((owner ^ 1) * rows + i * cut, across_cores(part)))
    return found


def scattered(left, right):
    size = lax.axis_size("fsdp")
    me = lax.axis_index("fsdp")
    rows = left.shape[1] // size
    contract_rows = (((0,), (0,)), ((), ()))

    def share(owner):
        columns = lax.dynamic_slice_in_dim(left, owner * rows, rows, 1)
        return lax.dot_general(
            columns, right, contract_rows, preferred_element_type=jnp.float32
        ).astype(jnp.bfloat16)

    order = list(range(1, size // 2)) + [0]
    given = [across_cores(share(((me ^ 1) + 2 * by) % size)) for by in order]
    total = None
    arrived = []
    for by, received in zip(order, given):
        own = share((me + 2 * by) % size).astype(jnp.float32) + received.astype(jnp.float32)
        if by:
            arrived.append(across_chips(own.astype(jnp.bfloat16), by))
        else:
            total = own
    return total, arrived


def added(total, arrived):
    total = total.astype(jnp.float32)
    for received in arrived:
        total = total + received.astype(jnp.float32)
    return total


def normalize(inputs, gain_values):
    widened = inputs.astype(jnp.float32)
    inv_rms = lax.rsqrt(jnp.mean(widened * widened, axis=-1, keepdims=True) + rms_eps)
    normed = (widened * inv_rms * gain_values).astype(jnp.bfloat16)
    return (widened, inv_rms, normed)


def finish_grad(widened, inv_rms, gain_values, upstream, grad_normed):
    scaled = grad_normed * gain_values
    inner_mean = jnp.mean(scaled * widened, axis=-1, keepdims=True)
    result = upstream.astype(jnp.float32) + inv_rms * scaled - widened * inv_rms**3 * inner_mean
    return result.astype(jnp.bfloat16)


def local(
    layer_inputs, out_grads, attn_stash, proj_grads, w_qkv, w_out, norm_gain, b_sched, w_sched
):
    seq_len, width = layer_inputs.shape[2:]
    cosine_table, sine_table = pair_tables(seq_len)
    gain_values = norm_gain[0]
    b_slot = b_sched[0]
    w_slot = w_sched[0]
    contract_cols = (((1,), (1,)), ((), ()))
    out_pieces = gathered(w_out[0], 1)
    qkv_pieces = gathered(w_qkv[0], 2)
    inputs_w = lax.dynamic_index_in_dim(layer_inputs[0], w_slot, 0, keepdims=False)
    upstream_w = lax.dynamic_index_in_dim(out_grads[0], w_slot, 0, keepdims=False)
    attended_w = lax.dynamic_index_in_dim(attn_stash[0], w_slot, 0, keepdims=False)
    projected_w = lax.dynamic_index_in_dim(proj_grads[0], w_slot, 0, keepdims=False)
    unused_wide, unused_inv, normed_w = normalize(inputs_w, gain_values)
    own_out, arrived_out = scattered(attended_w, upstream_w)
    own_qkv, arrived_qkv = scattered(normed_w, projected_w)
    inputs_b = lax.dynamic_index_in_dim(layer_inputs[0], b_slot, 0, keepdims=False)
    upstream_b = lax.dynamic_index_in_dim(out_grads[0], b_slot, 0, keepdims=False)
    widened, inv_rms, normed = normalize(inputs_b, gain_values)
    attn_grad = jnp.zeros((seq_len, HEADS * HEAD_DIM), jnp.bfloat16)
    for start, piece in out_pieces:
        block = lax.dot_general(
            upstream_b, piece, contract_cols, preferred_element_type=jnp.float32
        ).astype(jnp.bfloat16)
        attn_grad = lax.dynamic_update_slice(attn_grad, block, (0, start))
    qkv_rows = None
    early = len(qkv_pieces) - 2
    for number, (start, piece) in enumerate(qkv_pieces):
        if number == early:
            piece, qkv_rows, attn_grad, own_out, own_qkv = lax.optimization_barrier(
                (piece, qkv_rows, attn_grad, own_out, own_qkv)
            )
            qkv_pieces[number] = (start, piece)
        columns = lax.dynamic_slice_in_dim(normed, start, piece.shape[0], 1)
        term = jnp.dot(columns, piece, preferred_element_type=jnp.float32)
        qkv_rows = term if qkv_rows is None else qkv_rows + term
    grad_proj = attention_back(qkv_rows, attn_grad, cosine_table, sine_table)
    grad_normed = jnp.zeros((seq_len, width), jnp.float32)
    for start, piece in qkv_pieces:
        block = lax.dot_general(
            grad_proj, piece, contract_cols, preferred_element_type=jnp.float32
        )
        grad_normed = lax.dynamic_update_slice(grad_normed, block, (0, start))
    sent_grads = finish_grad(widened, inv_rms, gain_values, upstream_b, grad_normed)
    sent_back = passed_along(sent_grads, "section", -1)[None]
    return (sent_back, added(own_qkv, arrived_qkv)[None], added(own_out, arrived_out)[None])


def solution(mesh):
    return jax.shard_map(
        local,
        mesh=mesh,
        in_specs=(
            P("section", None, "fsdp", None),
            P("section", None, "fsdp", None),
            P("section", None, "fsdp", None),
            P("section", None, "fsdp", None),
            P("section", "fsdp", None),
            P("section", "fsdp", None),
            P("section", None),
            P("section"),
            P("section"),
        ),
        out_specs=(
            P("section", "fsdp", None),
            P("section", "fsdp", None),
            P("section", "fsdp", None),
        ),
        check_vma=False,
    )
```
